32 devices in a mesh: dp: 4 (over x, y), tp: 8 (over z, core).
Axes of the slice: x: 2, y: 2, z: 4, core: 2. Of those that a mesh axis runs over, the one named last changes fastest.
Arguments:
- x: bfloat16 [7168, 5120], P(('dp', 'tp')), parts along dimension 0
- w_gate: bfloat16 [5120, 12288], P(None, 'tp')
- w_up: bfloat16 [5120, 12288], P(None, 'tp')
- w_down: bfloat16 [12288, 5120], P('tp')
Outputs:
- output: bfloat16 [7168, 5120], P(('dp', 'tp')), parts along dimension 0
There are 4 independent parts. The reference program is written for one: setup_inputs(seed, part) draws one part's arguments, and reference() takes and returns one part's arrays. A program takes and returns all parts, laid end to end along the dimension named above; an argument that names none is the same for every part.
All inputs are finite; a program needn't handle non-finite values.
Results may differ from the reference program's by a relative error of at most 0.016.
Values are sent between devices in bfloat16 or wider.
A program may use at most 2 GiB of HBM per device.

```python
import jax
import jax.numpy as jnp

ROWS = 1792
D = 5120
FF = 12288


def setup_inputs(seed: int = 0, part: int = 0) -> dict:
    kx, kg, ku, kd = jax.random.split(jax.random.key(seed), 4)
    drawn = {
        "x": jax.random.normal(jax.random.fold_in(kx, part), (ROWS, D), jnp.float32),
        "w_gate": jax.random.normal(kg, (D, FF), jnp.float32) * D**-0.5,
        "w_up": jax.random.normal(ku, (D, FF), jnp.float32) * D**-0.5,
        "w_down": jax.random.normal(kd, (FF, D), jnp.float32) * FF**-0.5,
    }
    return {k: v.astype(jnp.bfloat16) for k, v in drawn.items()}


def reference(x, w_gate, w_up, w_down):
    gate = jnp.dot(x, w_gate, preferred_element_type=jnp.float32)
    up = jnp.dot(x, w_up, preferred_element_type=jnp.float32)
    hidden = (jax.nn.silu(gate) * up).astype(jnp.bfloat16)
    return jnp.dot(hidden, w_down, preferred_element_type=jnp.float32).astype(jnp.bfloat16)
```

```python
import jax
import jax.numpy as jnp
from jax import lax
from jax.experimental import pallas as pl
from jax.experimental.pallas import tpu as pltpu
from jax.sharding import PartitionSpec as P

MESH = pl.DeviceIdType.MESH
CHIPS = 4
SUBS = 2
CHUNKS = 10
LAG = 3
RING = 4
TILES = 3


def kernel(
    x, wg, wu, wd, y, xg,
    wgv, wuv, wdv, xb, hid, rin, own0, snd, term, give, take,
    ag_s, ag_r, dd_s, dd_r, os, orr, rin_r, own_r, snd_s, give_s, take_r, y_s, w_s, x_s, credit,
):
    f32, bf16 = jnp.float32, jnp.bfloat16
    half, depth = x.shape[0] // 2, x.shape[1]
    piece, width, tile = half // SUBS, depth // CHUNKS, wg.shape[1] // TILES
    t = lax.axis_index("tp")
    z, c = t // 2, t % 2
    other = t + 1 - 2 * c
    pos = (z, CHIPS - 1 - z)
    ahead, behind = (t + 2, t - 2), (t - 2, t + 2)
    inner = jnp.minimum(z, CHIPS - 1 - z)
    low = z < 2

    def remote(src, dst, send, recv, device):
        return pltpu.make_async_remote_copy(
            src_ref=src, dst_ref=dst, send_sem=send, recv_sem=recv, device_id={"tp": device}, device_id_type=MESH
        )

    def slab(j, h, core):
        return (j * 2 + h) * 2 + core

    def rows(i):
        return pl.ds(i * piece, piece)

    def cols(i, n):
        return pl.ds(pl.multiple_of(i * n, n), n)

    barrier = pltpu.get_barrier_semaphore()
    pl.semaphore_signal(barrier, inc=1, device_id={"tp": other}, device_id_type=MESH)
    for d in range(2):
        @pl.when(pos[d] < CHIPS - 1)
        def _():
            pl.semaphore_signal(barrier, inc=1, device_id={"tp": ahead[d]}, device_id_type=MESH)
    pl.semaphore_wait(barrier, 1 + jnp.minimum(z, 1) + jnp.minimum(CHIPS - 1 - z, 1))

    def send_own(d, h, slot, i):
        return remote(
            x.at[pl.ds(h * half + i * piece, piece)], xg.at[slab(z, h, c), rows(i)],
            ag_s.at[d, slot, i], ag_r.at[d, slot, i], ahead[d],
        )

    def give_own(h):
        return remote(x.at[pl.ds(h * half, half)], xg.at[slab(z, h, c)], os.at[h], orr.at[h], other)

    for d in range(2):
        @pl.when(pos[d] < CHIPS - 1)
        def _():
            for i in range(SUBS):
                send_own(d, 0, 0, i).start()
    give_own(0).start()

    def weight(k, src, dst, i):
        return pltpu.make_async_copy(src.at[:, cols(i, tile)], dst.at[:, cols(i, tile)], w_s.at[k, i])

    for i in range(TILES):
        weight(0, wg, wgv, i).start()
        weight(1, wu, wuv, i).start()
    load_wd = pltpu.make_async_copy(wd, wdv, w_s.at[2, 0])
    load_wd.start()
    give_own(1).start()

    def hidden_slot(a):
        return jnp.where(a == 0, 0, 1 + (a - 1) % 3)

    def forward(s):
        far = CHIPS - 1 - inner
        j = jnp.where(s <= far, inner + s, inner + 2 * far + 1 - s)
        h = jnp.where(s <= far, 0, 1)
        near = s > 2 * far
        j = jnp.where(near, 0, j)
        h = jnp.where(near, s - 5, h)
        slot = jnp.where(near, s - 5, s - 1)
        j = jnp.where(low, j, CHIPS - 1 - j)
        came = jnp.where(low, 1, 0)
        came = jnp.where(near, 1 - came, came)
        mine = pltpu.make_async_copy(x.at[pl.ds(0, half)], xb.at[pl.ds(0, half)], x_s.at[0])
        theirs = pltpu.make_async_copy(xg.at[0], xb.at[pl.ds(half, half)], x_s.at[1])

        @pl.when((s == 0) | (s == 7))
        def _():
            ho = s // 7
            pltpu.make_async_copy(
                x.at[pl.ds(pl.multiple_of(ho * half, half), half)], xb.at[pl.ds(0, half)], x_s.at[0]
            ).start()
            give_own(ho).wait_recv()
            pltpu.make_async_copy(xg.at[slab(z, ho, 1 - c)], xb.at[pl.ds(half, half)], x_s.at[1]).start()

        @pl.when((s > 0) & (s < 7))
        def _():
            pltpu.make_async_copy(xg.at[slab(j, h, c)], xb.at[pl.ds(0, half)], x_s.at[0]).start()
            for i in range(SUBS):
                spot = xg.at[slab(j, h, 1 - c), rows(i)]
                remote(spot, spot, dd_s.at[came, slot, i], dd_r.at[came, slot, i], other).wait_recv()
            pltpu.make_async_copy(xg.at[slab(j, h, 1 - c)], xb.at[pl.ds(half, half)], x_s.at[1]).start()

        mine.wait()
        theirs.wait()
        hs = hidden_slot(s)

        @pl.loop(0, TILES)
        def _(i):
            @pl.when(s == 0)
            def _():
                weight(0, wg, wgv, i).wait()
                weight(1, wu, wuv, i).wait()

            gate = jnp.dot(xb[...], wgv[:, cols(i, tile)], preferred_element_type=f32)
            up = jnp.dot(xb[...], wuv[:, cols(i, tile)], preferred_element_type=f32)
            hid[hs, :, cols(i, tile)] = (jax.nn.silu(gate) * up).astype(bf16)

    def relay(s, i):
        for d in range(2):
            @pl.when((pos[d] > 0) & (s < 2 * pos[d]))
            def _():
                p = pos[d] - 1
                j = jnp.where(s <= p, p - s, s - p - 1)
                h = jnp.where(s <= p, 0, 1)
                spot = xg.at[slab(j if d == 0 else CHIPS - 1 - j, h, c), rows(i)]
                remote(spot, spot, ag_s.at[d, s, i], ag_r.at[d, s, i], ahead[d]).wait_recv()

                @pl.when(pos[d] < CHIPS - 1)
                def _():
                    remote(spot, spot, ag_s.at[d, s + 1, i], ag_r.at[d, s + 1, i], ahead[d]).start()

                remote(spot, spot, dd_s.at[d, s, i], dd_r.at[d, s, i], other).start()

    def exchange(b, i):
        return remote(give.at[b, i % RING], take.at[b, i], give_s.at[b, i % RING], take_r.at[b, i], other)

    def make_term(b, hs, i):
        value = jnp.dot(hid[hs], wdv[:, cols(i, width)], preferred_element_type=f32)
        term[b, i % RING] = value[:half]

        @pl.when(i >= RING)
        def _():
            exchange(b, i - RING).wait_send()

        give[b, i % RING] = value[half:].astype(bf16)
        exchange(b, i).start()

    def drain(b):
        for i in range(CHUNKS - RING, CHUNKS):
            exchange(b, i).wait_send()

    def to_ring(d, i):
        return remote(snd.at[d, i], rin.at[d, i], snd_s.at[d, i], rin_r.at[d, i], ahead[d])

    def to_own(d, i):
        return remote(snd.at[d, i], own0.at[d, i], snd_s.at[d, i], own_r.at[d, i], ahead[d])

    def scatter(s):
        active = [(pos[d] < CHIPS - 1) & (s >= 2 * pos[d] + 1) & (s < 7) for d in range(2)]

        @pl.when(active[0] | active[1])
        def _():
            @pl.loop(0, CHUNKS + LAG)
            def _(i):
                for d in range(2):
                    far = low if d == 0 else jnp.logical_not(low)

                    @pl.when(active[d] & (i < CHUNKS))
                    def _():
                        make_term(d, hidden_slot(s - jnp.where(far, 2 * inner, 0)), i)

                for d in range(2):
                    @pl.when(active[d] & (i >= LAG))
                    def _():
                        k = i - LAG
                        r = s - 2 * pos[d] - 1
                        exchange(d, k).wait_recv()

                        @pl.when(pos[d] > 0)
                        def _():
                            to_ring(d, k).wait_recv()
                            term[d, k % RING] = term[d, k % RING] + rin[d, k].astype(f32)
                            pl.semaphore_signal(credit.at[d], inc=1, device_id={"tp": behind[d]}, device_id_type=MESH)

                        @pl.when(r >= 1)
                        def _():
                            to_ring(d, k).wait_send()

                        snd[d, k] = (term[d, k % RING] + take[d, k].astype(f32)).astype(bf16)

                        @pl.when(r == 0)
                        def _():
                            to_own(d, k).start()

                        @pl.when(r >= 2)
                        def _():
                            pl.semaphore_wait(credit.at[d], 1)

                        @pl.when(r >= 1)
                        def _():
                            to_ring(d, k).start()

            for d in range(2):
                @pl.when(active[d])
                def _():
                    drain(d)

    def write(h, i):
        spot = (pl.ds(h * half, half), cols(i, width))
        return pltpu.make_async_copy(xb.at[spot], y.at[spot], y_s.at[h, i])

    def finish(h, hs):
        came, sems = (own0, own_r) if h == 0 else (rin, rin_r)

        @pl.loop(0, CHUNKS + LAG)
        def _(i):
            @pl.when(i < CHUNKS)
            def _():
                make_term(h, hs, i)

            @pl.when(i >= LAG)
            def _():
                k = i - LAG
                exchange(h, k).wait_recv()
                term[h, k % RING] = term[h, k % RING] + take[h, k].astype(f32)
                for d in range(2):
                    @pl.when(pos[d] > 0)
                    def _():
                        remote(came.at[d, k], came.at[d, k], snd_s.at[d, k], sems.at[d, k], ahead[d]).wait_recv()
                        term[h, k % RING] = term[h, k % RING] + came[d, k].astype(f32)

                xb[pl.ds(h * half, half), cols(k, width)] = term[h, k % RING].astype(bf16)
                write(h, k).start()

        drain(h)

    @pl.loop(0, 8)
    def _(s):
        for d in range(2):
            @pl.when((pos[d] < CHIPS - 1) & (s == 2 * pos[d]))
            def _():
                for i in range(SUBS):
                    send_own(d, 1, s + 1, i).start()

        forward(s)

        @pl.when(s == 0)
        def _():
            load_wd.wait()

        relay(s, 0)
        scatter(s)
        for i in range(1, SUBS):
            relay(s, i)

    finish(0, 0)
    finish(1, 1)

    for h in range(2):
        give_own(h).wait_send()

        @pl.loop(0, CHUNKS)
        def _(i):
            write(h, i).wait()

    for d in range(2):
        for s in range(6):
            for i in range(SUBS):
                spot = xg.at[0, rows(i)]

                @pl.when((pos[d] < CHIPS - 1) & (s < 2 * pos[d] + 2))
                def _():
                    remote(spot, spot, ag_s.at[d, s, i], ag_r.at[d, s, i], ahead[d]).wait_send()

                @pl.when(s < 2 * pos[d])
                def _():
                    remote(spot, spot, dd_s.at[d, s, i], dd_r.at[d, s, i], other).wait_send()

        @pl.when(pos[d] < CHIPS - 1)
        def _():
            @pl.loop(0, CHUNKS)
            def _(i):
                to_ring(d, i).wait_send()


def block(x, w_gate, w_up, w_down):
    (n, depth), hidden = x.shape, w_gate.shape[1]
    half, width = n // 2, depth // CHUNKS
    f32, bf16, sem = jnp.float32, jnp.bfloat16, pltpu.SemaphoreType
    return pl.pallas_call(
        kernel,
        name="mlp_line",
        out_shape=(
            jax.ShapeDtypeStruct((n, depth), bf16),
            jax.ShapeDtypeStruct((4 * CHIPS, half, depth), bf16),
        ),
        in_specs=[pl.BlockSpec(memory_space=pl.ANY)] * 4,
        out_specs=(pl.BlockSpec(memory_space=pl.ANY),) * 2,
        scratch_shapes=[
            pltpu.VMEM((depth, hidden), bf16),
            pltpu.VMEM((depth, hidden), bf16),
            pltpu.VMEM((hidden, depth), bf16),
            pltpu.VMEM((n, depth), bf16),
            pltpu.VMEM((4, n, hidden), bf16),
            pltpu.VMEM((2, CHUNKS, half, width), bf16),
            pltpu.VMEM((2, CHUNKS, half, width), bf16),
            pltpu.VMEM((2, CHUNKS, half, width), bf16),
            pltpu.VMEM((2, RING, half, width), f32),
            pltpu.VMEM((2, RING, half, width), bf16),
            pltpu.VMEM((2, CHUNKS, half, width), bf16),
            sem.DMA((2, 6, SUBS)),
            sem.DMA((2, 6, SUBS)),
            sem.DMA((2, 6, SUBS)),
            sem.DMA((2, 6, SUBS)),
            sem.DMA((2,)),
            sem.DMA((2,)),
            sem.DMA((2, CHUNKS)),
            sem.DMA((2, CHUNKS)),
            sem.DMA((2, CHUNKS)),
            sem.DMA((2, RING)),
            sem.DMA((2, CHUNKS)),
            sem.DMA((2, CHUNKS)),
            sem.DMA((3, TILES)),
            sem.DMA((2,)),
            sem.REGULAR((2,)),
        ],
        compiler_params=pltpu.CompilerParams(
            collective_id=0, has_side_effects=True, vmem_limit_bytes=67_043_328
        ),
    )(x, w_gate, w_up, w_down)[0]


def solution(mesh):
    return jax.shard_map(
        block,
        mesh=mesh,
        in_specs=(P(("dp", "tp"), None), P(None, "tp"), P(None, "tp"), P("tp", None)),
        out_specs=P(("dp", "tp"), None),
        check_vma=False,
    )
```

```python
import jax
import jax.numpy as jnp
from jax import lax
from jax.experimental import pallas as pl
from jax.experimental.pallas import tpu as pltpu
from jax.sharding import PartitionSpec as P

MESH = pl.DeviceIdType.MESH
CHIPS = 4
SUBS = 2
CHUNKS = 10
LAG = 3
HOLD = 2
RING = 4
GIVES = 3
TILES = 3


def kernel(
    x, wg, wu, wd, y, xg,
    wgv, wuv, wdv, xb, hid, rin, own0, snd, term, give, take,
    ag_s, ag_r, dd_s, dd_r, os, orr, rin_r, own_r, snd_s, give_s, take_r, y_s, w_s, x_s, credit,
):
    f32, bf16 = jnp.float32, jnp.bfloat16
    half, depth = x.shape[0] // 2, x.shape[1]
    piece, width, tile = half // SUBS, depth // CHUNKS, wg.shape[1] // TILES
    t = lax.axis_index("tp")
    z, c = t // 2, t % 2
    other = t + 1 - 2 * c
    pos = (z, CHIPS - 1 - z)
    ahead, behind = (t + 2, t - 2), (t - 2, t + 2)
    inner = jnp.minimum(z, CHIPS - 1 - z)
    low = z < 2

    def remote(src, dst, send, recv, device):
        return pltpu.make_async_remote_copy(
            src_ref=src, dst_ref=dst, send_sem=send, recv_sem=recv, device_id={"tp": device}, device_id_type=MESH
        )

    def slab(j, h, core):
        return (j * 2 + h) * 2 + core

    def rows(i):
        return pl.ds(i * piece, piece)

    def cols(i, n):
        return pl.ds(pl.multiple_of(i * n, n), n)

    def give_own(h):
        spot = xb.at[pl.ds(half, half)] if h == 0 else xg.at[slab(z, h, c)]
        return remote(x.at[pl.ds(h * half, half)], spot, os.at[h], orr.at[h], other)

    def load(src, i):
        return pltpu.make_async_copy(src, xb.at[pl.ds(i * half, half)], x_s.at[i])

    def weight(k, src, dst, i):
        return pltpu.make_async_copy(src.at[:, cols(i, tile)], dst.at[:, cols(i, tile)], w_s.at[k, i])

    load(x.at[pl.ds(0, half)], 0).start()
    for i in range(TILES):
        weight(0, wg, wgv, i).start()
        weight(1, wu, wuv, i).start()
    load_wd = pltpu.make_async_copy(wd, wdv, w_s.at[2, 0])
    load_wd.start()

    barrier = pltpu.get_barrier_semaphore()
    pl.semaphore_signal(barrier, inc=1, device_id={"tp": other}, device_id_type=MESH)
    for d in range(2):
        @pl.when(pos[d] < CHIPS - 1)
        def _():
            pl.semaphore_signal(barrier, inc=1, device_id={"tp": ahead[d]}, device_id_type=MESH)
    pl.semaphore_wait(barrier, 1 + jnp.minimum(z, 1) + jnp.minimum(CHIPS - 1 - z, 1))

    def send_own(d, h, slot, i):
        return remote(
            x.at[pl.ds(h * half + i * piece, piece)], xg.at[slab(z, h, c), rows(i)],
            ag_s.at[d, slot, i], ag_r.at[d, slot, i], ahead[d],
        )

    for d in range(2):
        @pl.when(pos[d] < CHIPS - 1)
        def _():
            for i in range(SUBS):
                send_own(d, 0, 0, i).start()
    give_own(0).start()
    give_own(1).start()

    def hidden_slot(a):
        return jnp.where(a < 2, a, 2 + (a - 2) % 3)

    def forward(n):
        s = n - 1
        far = CHIPS - 1 - inner
        j = jnp.where(s <= far, inner + s, inner + 2 * far + 1 - s)
        h = jnp.where(s <= far, 0, 1)
        near = s > 2 * far
        j = jnp.where(near, 0, j)
        h = jnp.where(near, s - 5, h)
        slot = jnp.where(near, s - 5, s - 1)
        j = jnp.where(low, j, CHIPS - 1 - j)
        came = jnp.where(low, 1, 0)
        came = jnp.where(near, 1 - came, came)

        @pl.when(n == 0)
        def _():
            give_own(0).wait_recv()

        @pl.when(n == 1)
        def _():
            load(x.at[pl.ds(half, half)], 0).start()
            give_own(1).wait_recv()
            load(xg.at[slab(z, 1, 1 - c)], 1).start()

        @pl.when(n > 1)
        def _():
            load(xg.at[slab(j, h, c)], 0).start()
            for i in range(SUBS):
                spot = xg.at[slab(j, h, 1 - c), rows(i)]
                remote(spot, spot, dd_s.at[came, slot, i], dd_r.at[came, slot, i], other).wait_recv()
            load(xg.at[slab(j, h, 1 - c)], 1).start()

        load(xg.at[0], 0).wait()

        @pl.when(n > 0)
        def _():
            load(xg.at[0], 1).wait()

        hs = hidden_slot(n)

        @pl.loop(0, TILES)
        def _(i):
            @pl.when(n == 0)
            def _():
                weight(0, wg, wgv, i).wait()
                weight(1, wu, wuv, i).wait()

            gate = jnp.dot(xb[...], wgv[:, cols(i, tile)], preferred_element_type=f32)
            up = jnp.dot(xb[...], wuv[:, cols(i, tile)], preferred_element_type=f32)
            hid[hs, :, cols(i, tile)] = (jax.nn.silu(gate) * up).astype(bf16)

    def relay(s, i):
        for d in range(2):
            @pl.when((s >= 0) & (s < 2 * pos[d]))
            def _():
                p = pos[d] - 1
                j = jnp.where(s <= p, p - s, s - p - 1)
                h = jnp.where(s <= p, 0, 1)
                spot = xg.at[slab(j if d == 0 else CHIPS - 1 - j, h, c), rows(i)]
                remote(spot, spot, ag_s.at[d, s, i], ag_r.at[d, s, i], ahead[d]).wait_recv()

                @pl.when(pos[d] < CHIPS - 1)
                def _():
                    remote(spot, spot, ag_s.at[d, s + 1, i], ag_r.at[d, s + 1, i], ahead[d]).start()

                remote(spot, spot, dd_s.at[d, s, i], dd_r.at[d, s, i], other).start()

    def exchange(b, i):
        return remote(give.at[b, i % GIVES], take.at[b, i], give_s.at[b, i % GIVES], take_r.at[b, i], other)

    def make_term(b, hs, i):
        value = jnp.dot(hid[hs], wdv[:, cols(i, width)], preferred_element_type=f32)
        term[b, i % RING] = value[:half]

        @pl.when(i >= GIVES)
        def _():
            exchange(b, i - GIVES).wait_send()

        give[b, i % GIVES] = value[half:].astype(bf16)
        exchange(b, i).start()

    def drain(b):
        for i in range(CHUNKS - GIVES, CHUNKS):
            exchange(b, i).wait_send()

    def to_ring(d, i):
        return remote(snd.at[d, i], rin.at[d, i], snd_s.at[d, i], rin_r.at[d, i], ahead[d])

    def to_own(d, i):
        return remote(snd.at[d, i], own0.at[d, i], snd_s.at[d, i], own_r.at[d, i], ahead[d])

    def scatter(s):
        active = [(pos[d] < CHIPS - 1) & (s >= 2 * pos[d] + 1) & (s < 7) for d in range(2)]

        @pl.when(active[0] | active[1])
        def _():
            @pl.loop(0, CHUNKS + LAG + HOLD)
            def _(i):
                for d in range(2):
                    far = low if d == 0 else jnp.logical_not(low)

                    @pl.when(active[d] & (i < CHUNKS))
                    def _():
                        make_term(d, hidden_slot(s + 1 - jnp.where(far, 2 * inner, 0)), i)

                for d in range(2):
                    @pl.when(active[d] & (i >= LAG) & (i < CHUNKS + LAG))
                    def _():
                        k = i - LAG
                        exchange(d, k).wait_recv()

                        @pl.when(pos[d] > 0)
                        def _():
                            to_ring(d, k).wait_recv()
                            term[d, k % RING] = term[d, k % RING] + rin[d, k].astype(f32)
                            pl.semaphore_signal(credit.at[d], inc=1, device_id={"tp": behind[d]}, device_id_type=MESH)

                for d in range(2):
                    @pl.when(active[d] & (i >= LAG) & (i < CHUNKS + LAG))
                    def _():
                        k = i - LAG

                        @pl.when(s - 2 * pos[d] - 1 >= 1)
                        def _():
                            to_ring(d, k).wait_send()

                        snd[d, k] = (term[d, k % RING] + take[d, k].astype(f32)).astype(bf16)

                for d in range(2):
                    @pl.when(active[d] & (i >= LAG + HOLD))
                    def _():
                        k = i - LAG - HOLD
                        r = s - 2 * pos[d] - 1

                        @pl.when(r == 0)
                        def _():
                            to_own(d, k).start()

                        @pl.when(r >= 2)
                        def _():
                            pl.semaphore_wait(credit.at[d], 1)

                        @pl.when(r >= 1)
                        def _():
                            to_ring(d, k).start()

            for d in range(2):
                @pl.when(active[d])
                def _():
                    drain(d)

    def write(h, i):
        spot = (pl.ds(h * half, half), cols(i, width))
        return pltpu.make_async_copy(xb.at[spot], y.at[spot], y_s.at[h, i])

    def finish(h, hs):
        came, sems = (own0, own_r) if h == 0 else (rin, rin_r)

        @pl.loop(0, CHUNKS + LAG)
        def _(i):
            @pl.when(i < CHUNKS)
            def _():
                make_term(h, hs, i)

            @pl.when(i >= LAG)
            def _():
                k = i - LAG
                exchange(h, k).wait_recv()
                term[h, k % RING] = term[h, k % RING] + take[h, k].astype(f32)
                for d in range(2):
                    @pl.when(pos[d] > 0)
                    def _():
                        remote(came.at[d, k], came.at[d, k], snd_s.at[d, k], sems.at[d, k], ahead[d]).wait_recv()
                        term[h, k % RING] = term[h, k % RING] + came[d, k].astype(f32)

                xb[pl.ds(h * half, half), cols(k, width)] = term[h, k % RING].astype(bf16)
                write(h, k).start()

        drain(h)

    @pl.loop(0, 8)
    def _(n):
        s = n - 1
        for d in range(2):
            @pl.when((pos[d] < CHIPS - 1) & (s == 2 * pos[d]))
            def _():
                for i in range(SUBS):
                    send_own(d, 1, s + 1, i).start()

        forward(n)

        @pl.when(n == 1)
        def _():
            load_wd.wait()

        relay(s, 0)
        scatter(s)
        for i in range(1, SUBS):
            relay(s, i)

    finish(0, 0)
    finish(1, 1)

    for h in range(2):
        give_own(h).wait_send()

        @pl.loop(0, CHUNKS)
        def _(i):
            write(h, i).wait()

    for d in range(2):
        for s in range(6):
            for i in range(SUBS):
                spot = xg.at[0, rows(i)]

                @pl.when((pos[d] < CHIPS - 1) & (s < 2 * pos[d] + 2))
                def _():
                    remote(spot, spot, ag_s.at[d, s, i], ag_r.at[d, s, i], ahead[d]).wait_send()

                @pl.when(s < 2 * pos[d])
                def _():
                    remote(spot, spot, dd_s.at[d, s, i], dd_r.at[d, s, i], other).wait_send()

        @pl.when(pos[d] < CHIPS - 1)
        def _():
            @pl.loop(0, CHUNKS)
            def _(i):
                to_ring(d, i).wait_send()


def block(x, w_gate, w_up, w_down):
    (n, depth), hidden = x.shape, w_gate.shape[1]
    half, width = n // 2, depth // CHUNKS
    f32, bf16, sem = jnp.float32, jnp.bfloat16, pltpu.SemaphoreType
    return pl.pallas_call(
        kernel,
        name="mlp_line",
        out_shape=(
            jax.ShapeDtypeStruct((n, depth), bf16),
            jax.ShapeDtypeStruct((4 * CHIPS, half, depth), bf16),
        ),
        in_specs=[pl.BlockSpec(memory_space=pl.ANY)] * 4,
        out_specs=(pl.BlockSpec(memory_space=pl.ANY),) * 2,
        scratch_shapes=[
            pltpu.VMEM((depth, hidden), bf16),
            pltpu.VMEM((depth, hidden), bf16),
            pltpu.VMEM((hidden, depth), bf16),
            pltpu.VMEM((n, depth), bf16),
            pltpu.VMEM((5, n, hidden), bf16),
            pltpu.VMEM((2, CHUNKS, half, width), bf16),
            pltpu.VMEM((2, CHUNKS, half, width), bf16),
            pltpu.VMEM((2, CHUNKS, half, width), bf16),
            pltpu.VMEM((2, RING, half, width), f32),
            pltpu.VMEM((2, GIVES, half, width), bf16),
            pltpu.VMEM((2, CHUNKS, half, width), bf16),
            sem.DMA((2, 6, SUBS)),
            sem.DMA((2, 6, SUBS)),
            sem.DMA((2, 6, SUBS)),
            sem.DMA((2, 6, SUBS)),
            sem.DMA((2,)),
            sem.DMA((2,)),
            sem.DMA((2, CHUNKS)),
            sem.DMA((2, CHUNKS)),
            sem.DMA((2, CHUNKS)),
            sem.DMA((2, GIVES)),
            sem.DMA((2, CHUNKS)),
            sem.DMA((2, CHUNKS)),
            sem.DMA((3, TILES)),
            sem.DMA((2,)),
            sem.REGULAR((2,)),
        ],
        compiler_params=pltpu.CompilerParams(
            collective_id=0, has_side_effects=True, vmem_limit_bytes=67_043_328
        ),
    )(x, w_gate, w_up, w_down)[0]


def solution(mesh):
    return jax.shard_map(
        block,
        mesh=mesh,
        in_specs=(P(("dp", "tp"), None), P(None, "tp"), P(None, "tp"), P("tp", None)),
        out_specs=P(("dp", "tp"), None),
        check_vma=False,
    )
```

```python
import jax
import jax.numpy as jnp
from jax import lax
from jax.experimental import pallas as pl
from jax.experimental.pallas import tpu as pltpu
from jax.sharding import PartitionSpec as P

MESH = pl.DeviceIdType.MESH
CHIPS = 4
SUBS = 2
CHUNKS = 10
LAG = 3
HOLD = 2
RING = 4
GIVES = 3
TILES = 3


def kernel(
    x, wg, wu, wd, xb, xg,
    wgv, wuv, wdv, hid, rin, own0, snd, term, give, take,
    ag_s, ag_r, dd_s, dd_r, os, orr, rin_r, own_r, snd_s, give_s, take_r, w_s, x_s, credit,
):
    f32, bf16 = jnp.float32, jnp.bfloat16
    half, depth = x.shape[0] // 2, x.shape[1]
    piece, width, tile = half // SUBS, depth // CHUNKS, wg.shape[1] // TILES
    t = lax.axis_index("tp")
    z, c = t // 2, t % 2
    other = t + 1 - 2 * c
    pos = (z, CHIPS - 1 - z)
    ahead, behind = (t + 2, t - 2), (t - 2, t + 2)
    inner = jnp.minimum(z, CHIPS - 1 - z)
    low = z < 2

    def remote(src, dst, send, recv, device):
        return pltpu.make_async_remote_copy(
            src_ref=src, dst_ref=dst, send_sem=send, recv_sem=recv, device_id={"tp": device}, device_id_type=MESH
        )

    def slab(j, h, core):
        return (j * 2 + h) * 2 + core

    def rows(i):
        return pl.ds(i * piece, piece)

    def cols(i, n):
        return pl.ds(pl.multiple_of(i * n, n), n)

    def give_own(h):
        spot = xb.at[pl.ds(half, half)] if h == 0 else xg.at[slab(z, h, c)]
        return remote(x.at[pl.ds(h * half, half)], spot, os.at[h], orr.at[h], other)

    def load(src, i):
        return pltpu.make_async_copy(src, xb.at[pl.ds(i * half, half)], x_s.at[i])

    def weight(k, src, dst, i):
        return pltpu.make_async_copy(src.at[:, cols(i, tile)], dst.at[:, cols(i, tile)], w_s.at[k, i])

    load(x.at[pl.ds(0, half)], 0).start()
    for i in range(TILES):
        weight(0, wg, wgv, i).start()
        weight(1, wu, wuv, i).start()
    load_wd = pltpu.make_async_copy(wd, wdv, w_s.at[2, 0])
    load_wd.start()

    barrier = pltpu.get_barrier_semaphore()
    pl.semaphore_signal(barrier, inc=1, device_id={"tp": other}, device_id_type=MESH)
    for d in range(2):
        @pl.when(pos[d] < CHIPS - 1)
        def _():
            pl.semaphore_signal(barrier, inc=1, device_id={"tp": ahead[d]}, device_id_type=MESH)
    pl.semaphore_wait(barrier, 1 + jnp.minimum(z, 1) + jnp.minimum(CHIPS - 1 - z, 1))

    def send_own(d, h, slot, i):
        return remote(
            x.at[pl.ds(h * half + i * piece, piece)], xg.at[slab(z, h, c), rows(i)],
            ag_s.at[d, slot, i], ag_r.at[d, slot, i], ahead[d],
        )

    for d in range(2):
        @pl.when(pos[d] < CHIPS - 1)
        def _():
            for i in range(SUBS):
                send_own(d, 0, 0, i).start()
    give_own(0).start()
    give_own(1).start()

    def hidden_slot(a):
        return jnp.where(a < 2, a, 2 + (a - 2) % 3)

    def forward(n):
        s = n - 1
        far = CHIPS - 1 - inner
        j = jnp.where(s <= far, inner + s, inner + 2 * far + 1 - s)
        h = jnp.where(s <= far, 0, 1)
        near = s > 2 * far
        j = jnp.where(near, 0, j)
        h = jnp.where(near, s - 5, h)
        slot = jnp.where(near, s - 5, s - 1)
        j = jnp.where(low, j, CHIPS - 1 - j)
        came = jnp.where(low, 1, 0)
        came = jnp.where(near, 1 - came, came)

        @pl.when(n == 0)
        def _():
            give_own(0).wait_recv()

        @pl.when(n == 1)
        def _():
            load(x.at[pl.ds(half, half)], 0).start()
            give_own(1).wait_recv()
            load(xg.at[slab(z, 1, 1 - c)], 1).start()

        @pl.when(n > 1)
        def _():
            load(xg.at[slab(j, h, c)], 0).start()
            for i in range(SUBS):
                spot = xg.at[slab(j, h, 1 - c), rows(i)]
                remote(spot, spot, dd_s.at[came, slot, i], dd_r.at[came, slot, i], other).wait_recv()
            load(xg.at[slab(j, h, 1 - c)], 1).start()

        load(xg.at[0], 0).wait()

        @pl.when(n > 0)
        def _():
            load(xg.at[0], 1).wait()

        hs = hidden_slot(n)

        @pl.loop(0, TILES)
        def _(i):
            @pl.when(n == 0)
            def _():
                weight(0, wg, wgv, i).wait()
                weight(1, wu, wuv, i).wait()

            gate = jnp.dot(xb[...], wgv[:, cols(i, tile)], preferred_element_type=f32)
            up = jnp.dot(xb[...], wuv[:, cols(i, tile)], preferred_element_type=f32)
            hid[hs, :, cols(i, tile)] = (jax.nn.silu(gate) * up).astype(bf16)

    def relay(s, i):
        for d in range(2):
            @pl.when((s >= 0) & (s < 2 * pos[d]))
            def _():
                p = pos[d] - 1
                j = jnp.where(s <= p, p - s, s - p - 1)
                h = jnp.where(s <= p, 0, 1)
                spot = xg.at[slab(j if d == 0 else CHIPS - 1 - j, h, c), rows(i)]
                remote(spot, spot, ag_s.at[d, s, i], ag_r.at[d, s, i], ahead[d]).wait_recv()

                @pl.when(pos[d] < CHIPS - 1)
                def _():
                    remote(spot, spot, ag_s.at[d, s + 1, i], ag_r.at[d, s + 1, i], ahead[d]).start()

                remote(spot, spot, dd_s.at[d, s, i], dd_r.at[d, s, i], other).start()

    def exchange(b, i):
        return remote(give.at[b, i % GIVES], take.at[b, i], give_s.at[b, i % GIVES], take_r.at[b, i], other)

    def make_term(b, hs, i):
        value = jnp.dot(hid[hs], wdv[:, cols(i, width)], preferred_element_type=f32)
        term[b, i % RING] = value[:half]

        @pl.when(i >= GIVES)
        def _():
            exchange(b, i - GIVES).wait_send()

        give[b, i % GIVES] = value[half:].astype(bf16)
        exchange(b, i).start()

    def drain(b):
        for i in range(CHUNKS - GIVES, CHUNKS):
            exchange(b, i).wait_send()

    def to_ring(d, i):
        return remote(snd.at[d, i], rin.at[d, i], snd_s.at[d, i], rin_r.at[d, i], ahead[d])

    def to_own(d, i):
        return remote(snd.at[d, i], own0.at[d, i], snd_s.at[d, i], own_r.at[d, i], ahead[d])

    def scatter(s):
        active = [(pos[d] < CHIPS - 1) & (s >= 2 * pos[d] + 1) & (s < 7) for d in range(2)]

        @pl.when(active[0] | active[1])
        def _():
            @pl.loop(0, CHUNKS + LAG + HOLD)
            def _(i):
                for d in range(2):
                    far = low if d == 0 else jnp.logical_not(low)

                    @pl.when(active[d] & (i < CHUNKS))
                    def _():
                        make_term(d, hidden_slot(s + 1 - jnp.where(far, 2 * inner, 0)), i)

                for d in range(2):
                    @pl.when(active[d] & (i >= LAG) & (i < CHUNKS + LAG))
                    def _():
                        k = i - LAG
                        exchange(d, k).wait_recv()

                        @pl.when(pos[d] > 0)
                        def _():
                            to_ring(d, k).wait_recv()
                            term[d, k % RING] = term[d, k % RING] + rin[d, k].astype(f32)
                            pl.semaphore_signal(credit.at[d], inc=1, device_id={"tp": behind[d]}, device_id_type=MESH)

                for d in range(2):
                    @pl.when(active[d] & (i >= LAG) & (i < CHUNKS + LAG))
                    def _():
                        k = i - LAG

                        @pl.when(s - 2 * pos[d] - 1 >= 1)
                        def _():
                            to_ring(d, k).wait_send()

                        snd[d, k] = (term[d, k % RING] + take[d, k].astype(f32)).astype(bf16)

                for d in range(2):
                    @pl.when(active[d] & (i >= LAG + HOLD))
                    def _():
                        k = i - LAG - HOLD
                        r = s - 2 * pos[d] - 1

                        @pl.when(r == 0)
                        def _():
                            to_own(d, k).start()

                        @pl.when(r >= 2)
                        def _():
                            pl.semaphore_wait(credit.at[d], 1)

                        @pl.when(r >= 1)
                        def _():
                            to_ring(d, k).start()

            for d in range(2):
                @pl.when(active[d])
                def _():
                    drain(d)

    def finish(h, hs):
        came, sems = (own0, own_r) if h == 0 else (rin, rin_r)

        @pl.loop(0, CHUNKS + LAG)
        def _(i):
            @pl.when(i < CHUNKS)
            def _():
                make_term(h, hs, i)

            @pl.when(i >= LAG)
            def _():
                k = i - LAG
                exchange(h, k).wait_recv()
                term[h, k % RING] = term[h, k % RING] + take[h, k].astype(f32)
                for d in range(2):
                    @pl.when(pos[d] > 0)
                    def _():
                        remote(came.at[d, k], came.at[d, k], snd_s.at[d, k], sems.at[d, k], ahead[d]).wait_recv()
                        term[h, k % RING] = term[h, k % RING] + came[d, k].astype(f32)

                xb[pl.ds(h * half, half), cols(k, width)] = term[h, k % RING].astype(bf16)

        drain(h)

    @pl.loop(0, 8)
    def _(n):
        s = n - 1
        for d in range(2):
            @pl.when((pos[d] < CHIPS - 1) & (s == 2 * pos[d]))
            def _():
                for i in range(SUBS):
                    send_own(d, 1, s + 1, i).start()

        forward(n)

        @pl.when(n == 1)
        def _():
            load_wd.wait()

        relay(s, 0)
        scatter(s)
        for i in range(1, SUBS):
            relay(s, i)

    for h in range(2):
        give_own(h).wait_send()
    for d in range(2):
        @pl.loop(0, 6)
        def _(s):
            for i in range(SUBS):
                spot = xg.at[0, rows(i)]

                @pl.when((pos[d] < CHIPS - 1) & (s < 2 * pos[d] + 2))
                def _():
                    remote(spot, spot, ag_s.at[d, s, i], ag_r.at[d, s, i], ahead[d]).wait_send()

                @pl.when(s < 2 * pos[d])
                def _():
                    remote(spot, spot, dd_s.at[d, s, i], dd_r.at[d, s, i], other).wait_send()

    finish(0, 0)
    finish(1, 1)
    for d in range(2):
        @pl.when(pos[d] < CHIPS - 1)
        def _():
            @pl.loop(0, CHUNKS)
            def _(i):
                to_ring(d, i).wait_send()


def block(x, w_gate, w_up, w_down):
    (n, depth), hidden = x.shape, w_gate.shape[1]
    half, width = n // 2, depth // CHUNKS
    f32, bf16, sem = jnp.float32, jnp.bfloat16, pltpu.SemaphoreType
    return pl.pallas_call(
        kernel,
        name="mlp_line",
        out_shape=(
            pltpu.VMEM((n, depth), bf16),
            jax.ShapeDtypeStruct((4 * CHIPS, half, depth), bf16),
        ),
        in_specs=[pl.BlockSpec(memory_space=pl.ANY)] * 4,
        out_specs=(pl.BlockSpec(memory_space=pltpu.VMEM), pl.BlockSpec(memory_space=pl.ANY)),
        scratch_shapes=[
            pltpu.VMEM((depth, hidden), bf16),
            pltpu.VMEM((depth, hidden), bf16),
            pltpu.VMEM((hidden, depth), bf16),
            pltpu.VMEM((5, n, hidden), bf16),
            pltpu.VMEM((2, CHUNKS, half, width), bf16),
            pltpu.VMEM((2, CHUNKS, half, width), bf16),
            pltpu.VMEM((2, CHUNKS, half, width), bf16),
            pltpu.VMEM((2, RING, half, width), f32),
            pltpu.VMEM((2, GIVES, half, width), bf16),
            pltpu.VMEM((2, CHUNKS, half, width), bf16),
            sem.DMA((2, 6, SUBS)),
            sem.DMA((2, 6, SUBS)),
            sem.DMA((2, 6, SUBS)),
            sem.DMA((2, 6, SUBS)),
            sem.DMA((2,)),
            sem.DMA((2,)),
            sem.DMA((2, CHUNKS)),
            sem.DMA((2, CHUNKS)),
            sem.DMA((2, CHUNKS)),
            sem.DMA((2, GIVES)),
            sem.DMA((2, CHUNKS)),
            sem.DMA((3, TILES)),
            sem.DMA((2,)),
            sem.REGULAR((2,)),
        ],
        compiler_params=pltpu.CompilerParams(
            collective_id=0, has_side_effects=True, vmem_limit_bytes=64_700_000
        ),
    )(x, w_gate, w_up, w_down)[0]


def solution(mesh):
    return jax.shard_map(
        block,
        mesh=mesh,
        in_specs=(P(("dp", "tp"), None), P(None, "tp"), P(None, "tp"), P("tp", None)),
        out_specs=P(("dp", "tp"), None),
        check_vma=False,
    )
```

```python
import jax
import jax.numpy as jnp
from jax import lax
from jax.experimental import pallas as pl
from jax.experimental.pallas import tpu as pltpu
from jax.sharding import PartitionSpec as P

MESH = pl.DeviceIdType.MESH
CHIPS = 4
SUBS = 2
CHUNKS = 10
LAG = 3
HOLD = 2
RING = 4
GIVES = 3
TILES = 3


def kernel(
    x, wg, wu, wd, xb, xg,
    wgv, wuv, wdv, hid, rin, own0, snd, term, give, take,
    ag_s, ag_r, dd_s, dd_r, os, orr, rin_r, own_r, snd_s, give_s, take_r, w_s, x_s, credit,
):
    f32, bf16 = jnp.float32, jnp.bfloat16
    half, depth = x.shape[0] // 2, x.shape[1]
    piece, width, tile = half // SUBS, depth // CHUNKS, wg.shape[1] // TILES
    t = lax.axis_index("tp")
    z, c = t // 2, t % 2
    other = t + 1 - 2 * c
    pos = (z, CHIPS - 1 - z)
    ahead, behind = (t + 2, t - 2), (t - 2, t + 2)
    inner = jnp.minimum(z, CHIPS - 1 - z)
    low = z < 2

    def remote(src, dst, send, recv, device):
        return pltpu.make_async_remote_copy(
            src_ref=src, dst_ref=dst, send_sem=send, recv_sem=recv, device_id={"tp": device}, device_id_type=MESH
        )

    def slab(j, h, core):
        return (j * 2 + h) * 2 + core

    def rows(i):
        return pl.ds(i * piece, piece)

    def cols(i, n):
        return pl.ds(pl.multiple_of(i * n, n), n)

    def give_own(h):
        spot = xb.at[pl.ds(half, half)] if h == 0 else xg.at[slab(z, h, c)]
        return remote(x.at[pl.ds(h * half, half)], spot, os, orr.at[h], other)

    def load(src, i):
        return pltpu.make_async_copy(src, xb.at[pl.ds(i * half, half)], x_s.at[i])

    def weight(k, src, dst, i):
        return pltpu.make_async_copy(src.at[:, cols(i, tile)], dst.at[:, cols(i, tile)], w_s.at[k * TILES + i])

    barrier = pltpu.get_barrier_semaphore()
    pl.semaphore_signal(barrier, inc=1, device_id={"tp": other}, device_id_type=MESH)
    for d in range(2):
        @pl.when(pos[d] < CHIPS - 1)
        def _():
            pl.semaphore_signal(barrier, inc=1, device_id={"tp": ahead[d]}, device_id_type=MESH)

    load(x.at[pl.ds(0, half)], 0).start()
    for i in range(TILES):
        weight(0, wg, wgv, i).start()
        weight(1, wu, wuv, i).start()
    load_wd = pltpu.make_async_copy(wd, wdv, w_s.at[2 * TILES])
    load_wd.start()
    pl.semaphore_wait(barrier, 1 + jnp.minimum(z, 1) + jnp.minimum(CHIPS - 1 - z, 1))

    def send_own(d, h, slot, i):
        return remote(
            x.at[pl.ds(h * half + i * piece, piece)], xg.at[slab(z, h, c), rows(i)],
            ag_s.at[d], ag_r.at[d, slot, i], ahead[d],
        )

    for d in range(2):
        @pl.when(pos[d] < CHIPS - 1)
        def _():
            for i in range(SUBS):
                send_own(d, 0, 0, i).start()
    give_own(0).start()
    give_own(1).start()

    def hidden_slot(a):
        return jnp.where(a < 2, a, 2 + (a - 2) % 3)

    def forward(n):
        s = n - 1
        far = CHIPS - 1 - inner
        j = jnp.where(s <= far, inner + s, inner + 2 * far + 1 - s)
        h = jnp.where(s <= far, 0, 1)
        near = s > 2 * far
        j = jnp.where(near, 0, j)
        h = jnp.where(near, s - 5, h)
        slot = jnp.where(near, s - 5, s - 1)
        j = jnp.where(low, j, CHIPS - 1 - j)
        came = jnp.where(low, 1, 0)
        came = jnp.where(near, 1 - came, came)

        @pl.when(n == 0)
        def _():
            give_own(0).wait_recv()

        @pl.when(n == 1)
        def _():
            load(x.at[pl.ds(half, half)], 0).start()
            give_own(1).wait_recv()
            load(xg.at[slab(z, 1, 1 - c)], 1).start()

        @pl.when(n > 1)
        def _():
            load(xg.at[slab(j, h, c)], 0).start()
            spot = xg.at[slab(j, h, 1 - c)]
            remote(spot, spot, dd_s.at[came], dd_r.at[came, slot], other).wait_recv()
            load(spot, 1).start()

        load(xg.at[0], 0).wait()

        @pl.when(n > 0)
        def _():
            load(xg.at[0], 1).wait()

        hs = hidden_slot(n)

        @pl.loop(0, TILES)
        def _(i):
            @pl.when(n == 0)
            def _():
                weight(0, wg, wgv, i).wait()
                weight(1, wu, wuv, i).wait()

            gate = jnp.dot(xb[...], wgv[:, cols(i, tile)], preferred_element_type=f32)
            up = jnp.dot(xb[...], wuv[:, cols(i, tile)], preferred_element_type=f32)
            hid[hs, :, cols(i, tile)] = (jax.nn.silu(gate) * up).astype(bf16)

    def relay(s, i):
        for d in range(2):
            @pl.when((s >= 0) & (s < 2 * pos[d]))
            def _():
                p = pos[d] - 1
                j = jnp.where(s <= p, p - s, s - p - 1)
                h = jnp.where(s <= p, 0, 1)
                spot = xg.at[slab(j if d == 0 else CHIPS - 1 - j, h, c), rows(i)]
                remote(spot, spot, ag_s.at[d], ag_r.at[d, s, i], ahead[d]).wait_recv()

                @pl.when(pos[d] < CHIPS - 1)
                def _():
                    remote(spot, spot, ag_s.at[d], ag_r.at[d, s + 1, i], ahead[d]).start()

                remote(spot, spot, dd_s.at[d], dd_r.at[d, s], other).start()

    def exchange(b, i):
        return remote(give.at[b, i % GIVES], take.at[b, i], give_s.at[b, i % GIVES], take_r.at[b, i], other)

    def make_term(b, hs, i):
        value = jnp.dot(hid[hs], wdv[:, cols(i, width)], preferred_element_type=f32)
        term[b, i % RING] = value[:half]

        @pl.when(i >= GIVES)
        def _():
            exchange(b, i - GIVES).wait_send()

        give[b, i % GIVES] = value[half:].astype(bf16)
        exchange(b, i).start()

    def drain(b):
        for i in range(CHUNKS - GIVES, CHUNKS):
            exchange(b, i).wait_send()

    def to_ring(d, i):
        return remote(snd.at[d, i], rin.at[d, i], snd_s.at[d, i], rin_r.at[d, i], ahead[d])

    def to_own(d, i):
        return remote(snd.at[d, i], own0.at[d, i], snd_s.at[d, i], own_r.at[d], ahead[d])

    def scatter(s):
        active = [(pos[d] < CHIPS - 1) & (s >= 2 * pos[d] + 1) & (s < 7) for d in range(2)]

        @pl.when(active[0] | active[1])
        def _():
            @pl.loop(0, CHUNKS + LAG + HOLD)
            def _(i):
                for d in range(2):
                    far = low if d == 0 else jnp.logical_not(low)

                    @pl.when(active[d] & (i < CHUNKS))
                    def _():
                        make_term(d, hidden_slot(s + 1 - jnp.where(far, 2 * inner, 0)), i)

                for d in range(2):
                    @pl.when(active[d] & (i >= LAG) & (i < CHUNKS + LAG))
                    def _():
                        k = i - LAG
                        exchange(d, k).wait_recv()

                        @pl.when(pos[d] > 0)
                        def _():
                            to_ring(d, k).wait_recv()
                            term[d, k % RING] = term[d, k % RING] + rin[d, k].astype(f32)
                            pl.semaphore_signal(credit.at[d], inc=1, device_id={"tp": behind[d]}, device_id_type=MESH)

                for d in range(2):
                    @pl.when(active[d] & (i >= LAG) & (i < CHUNKS + LAG))
                    def _():
                        k = i - LAG

                        @pl.when(s - 2 * pos[d] - 1 >= 1)
                        def _():
                            to_ring(d, k).wait_send()

                        snd[d, k] = (term[d, k % RING] + take[d, k].astype(f32)).astype(bf16)

                for d in range(2):
                    @pl.when(active[d] & (i >= LAG + HOLD))
                    def _():
                        k = i - LAG - HOLD
                        r = s - 2 * pos[d] - 1

                        @pl.when(r == 0)
                        def _():
                            to_own(d, k).start()

                        @pl.when(r >= 2)
                        def _():
                            pl.semaphore_wait(credit.at[d], 1)

                        @pl.when(r >= 1)
                        def _():
                            to_ring(d, k).start()

            for d in range(2):
                @pl.when(active[d])
                def _():
                    drain(d)

    def finish(h, hs):
        came = own0 if h == 0 else rin
        if h == 0:
            for d in range(2):
                @pl.when(pos[d] > 0)
                def _():
                    remote(own0.at[d], own0.at[d], snd_s.at[d, 0], own_r.at[d], ahead[d]).wait_recv()

        @pl.loop(0, CHUNKS + LAG)
        def _(i):
            @pl.when(i < CHUNKS)
            def _():
                make_term(h, hs, i)

            @pl.when(i >= LAG)
            def _():
                k = i - LAG
                exchange(h, k).wait_recv()
                term[h, k % RING] = term[h, k % RING] + take[h, k].astype(f32)
                for d in range(2):
                    @pl.when(pos[d] > 0)
                    def _():
                        if h == 1:
                            to_ring(d, k).wait_recv()
                        term[h, k % RING] = term[h, k % RING] + came[d, k].astype(f32)

                xb[pl.ds(h * half, half), cols(k, width)] = term[h, k % RING].astype(bf16)

        drain(h)

    @pl.loop(0, 8)
    def _(n):
        s = n - 1
        for d in range(2):
            @pl.when((pos[d] < CHIPS - 1) & (s == 2 * pos[d]))
            def _():
                for i in range(SUBS):
                    send_own(d, 1, s + 1, i).start()

        @pl.when(n == 1)
        def _():
            relay(0, 0)

        forward(n)

        @pl.when(n == 1)
        def _():
            load_wd.wait()

        @pl.when(n > 1)
        def _():
            relay(s, 0)

        scatter(s)
        for i in range(1, SUBS):
            relay(s, i)

    pltpu.make_async_copy(x, x, os).wait()
    for d in range(2):
        for p in range(CHIPS):
            @pl.when(pos[d] == p)
            def _():
                if p < CHIPS - 1:
                    spot = xg.at[pl.ds(0, 2 * p + 2)]
                    remote(spot, spot, ag_s.at[d], ag_r.at[d, 0, 0], ahead[d]).wait_send()
                if p > 0:
                    spot = xg.at[pl.ds(0, 2 * p)]
                    remote(spot, spot, dd_s.at[d], dd_r.at[d, 0], other).wait_send()

    finish(0, 0)
    finish(1, 1)
    for d in range(2):
        @pl.when(pos[d] < CHIPS - 1)
        def _():
            @pl.loop(0, CHUNKS)
            def _(i):
                to_ring(d, i).wait_send()


def block(x, w_gate, w_up, w_down):
    (n, depth), hidden = x.shape, w_gate.shape[1]
    half, width = n // 2, depth // CHUNKS
    f32, bf16, sem = jnp.float32, jnp.bfloat16, pltpu.SemaphoreType
    return pl.pallas_call(
        kernel,
        name="mlp_line",
        out_shape=(
            pltpu.VMEM((n, depth), bf16),
            jax.ShapeDtypeStruct((4 * CHIPS, half, depth), bf16),
        ),
        in_specs=[pl.BlockSpec(memory_space=pl.ANY)] * 4,
        out_specs=(pl.BlockSpec(memory_space=pltpu.VMEM), pl.BlockSpec(memory_space=pl.ANY)),
        scratch_shapes=[
            pltpu.VMEM((depth, hidden), bf16),
            pltpu.VMEM((depth, hidden), bf16),
            pltpu.VMEM((hidden, depth), bf16),
            pltpu.VMEM((5, n, hidden), bf16),
            pltpu.VMEM((2, CHUNKS, half, width), bf16),
            pltpu.VMEM((2, CHUNKS, half, width), bf16),
            pltpu.VMEM((2, CHUNKS, half, width), bf16),
            pltpu.VMEM((2, RING, half, width), f32),
            pltpu.VMEM((2, GIVES, half, width), bf16),
            pltpu.VMEM((2, CHUNKS, half, width), bf16),
            sem.DMA((2,)),
            sem.DMA((2, 6, SUBS)),
            sem.DMA((2,)),
            sem.DMA((2, 6)),
            sem.DMA,
            sem.DMA((2,)),
            sem.DMA((2, CHUNKS)),
            sem.DMA((2,)),
            sem.DMA((2, CHUNKS)),
            sem.DMA((2, GIVES)),
            sem.DMA((2, CHUNKS)),
            sem.DMA((2 * TILES + 1,)),
            sem.DMA((2,)),
            sem.REGULAR((2,)),
        ],
        compiler_params=pltpu.CompilerParams(
            collective_id=0, has_side_effects=True, vmem_limit_bytes=64_700_000
        ),
    )(x, w_gate, w_up, w_down)[0]


def solution(mesh):
    return jax.shard_map(
        block,
        mesh=mesh,
        in_specs=(P(("dp", "tp"), None), P(None, "tp"), P(None, "tp"), P("tp", None)),
        out_specs=P(("dp", "tp"), None),
        check_vma=False,
    )
```

```python
import jax
import jax.numpy as jnp
from jax import lax
from jax.experimental import pallas as pl
from jax.experimental.pallas import tpu as pltpu
from jax.sharding import PartitionSpec as P

MESH = pl.DeviceIdType.MESH
CHIPS = 4
SUBS = 2
CHUNKS = 10
LAG = 3
HOLD = 2
RING = 4
GIVES = 3
TILES = 3


def kernel(
    x, wg, wu, wd, xb, xg,
    wgv, wuv, wdv, hid, rin, own0, snd, term, give, take,
    ag_s, ag_r, dd_s, dd_r, os, orr, rin_r, own_r, snd_s, give_s, take_r, w_s, x_s, credit, hello,
):
    f32, bf16 = jnp.float32, jnp.bfloat16
    half, depth = x.shape[0] // 2, x.shape[1]
    piece, width, tile = half // SUBS, depth // CHUNKS, wg.shape[1] // TILES
    t = lax.axis_index("tp")
    z, c = t // 2, t % 2
    other = t + 1 - 2 * c
    pos = (z, CHIPS - 1 - z)
    ahead, behind = (t + 2, t - 2), (t - 2, t + 2)
    inner = jnp.minimum(z, CHIPS - 1 - z)
    low = z < 2

    def remote(src, dst, send, recv, device):
        return pltpu.make_async_remote_copy(
            src_ref=src, dst_ref=dst, send_sem=send, recv_sem=recv, device_id={"tp": device}, device_id_type=MESH
        )

    def slab(j, h, core):
        return (j * 2 + h) * 2 + core

    def place(d, slot):
        return slot if d == 0 else 2 * CHIPS - 3 - slot

    def rows(i):
        return pl.ds(i * piece, piece)

    def cols(i, n):
        return pl.ds(pl.multiple_of(i * n, n), n)

    def give_own(h):
        spot = xb.at[pl.ds(half, half)] if h == 0 else xg.at[slab(z, h, c)]
        return remote(x.at[pl.ds(h * half, half)], spot, os, orr.at[h], other)

    def load(src, i):
        return pltpu.make_async_copy(src, xb.at[pl.ds(i * half, half)], x_s.at[i])

    def weight(k, src, dst, i):
        return pltpu.make_async_copy(src.at[:, cols(i, tile)], dst.at[:, cols(i, tile)], w_s.at[k * TILES + i])

    barrier = pltpu.get_barrier_semaphore()

    @pl.when(z < CHIPS - 1)
    def _():
        pl.semaphore_signal(barrier, inc=1, device_id={"tp": ahead[0]}, device_id_type=MESH)

    pl.semaphore_signal(barrier, inc=1, device_id={"tp": other}, device_id_type=MESH)
    load(x.at[pl.ds(0, half)], 0).start()
    for i in range(TILES):
        weight(0, wg, wgv, i).start()
        weight(1, wu, wuv, i).start()
    load_wd = pltpu.make_async_copy(wd, wdv, w_s.at[2 * TILES])
    load_wd.start()
    def send_own(d, h, slot, i):
        return remote(
            x.at[pl.ds(h * half + i * piece, piece)], xg.at[slab(z, h, c), rows(i)],
            ag_s.at[d], ag_r.at[place(d, slot), i], ahead[d],
        )

    pl.semaphore_wait(barrier, 1 + jnp.minimum(z, 1))

    @pl.when(z > 0)
    def _():
        pl.semaphore_signal(hello, inc=1, device_id={"tp": ahead[1]}, device_id_type=MESH)
        for i in range(SUBS):
            send_own(1, 0, 0, i).start()

    give_own(0).start()
    give_own(1).start()

    @pl.when(z < CHIPS - 1)
    def _():
        pl.semaphore_wait(hello, 1)
        for i in range(SUBS):
            send_own(0, 0, 0, i).start()


    def hidden_slot(a):
        return jnp.where(a < 2, a, 2 + (a - 2) % 3)

    def forward(n):
        s = n - 1
        far = CHIPS - 1 - inner
        j = jnp.where(s <= far, inner + s, inner + 2 * far + 1 - s)
        h = jnp.where(s <= far, 0, 1)
        near = s > 2 * far
        j = jnp.where(near, 0, j)
        h = jnp.where(near, s - 5, h)
        slot = jnp.where(near, s - 5, s - 1)
        j = jnp.where(low, j, CHIPS - 1 - j)
        came = jnp.where(low, 1, 0)
        came = jnp.where(near, 1 - came, came)

        @pl.when(n == 0)
        def _():
            give_own(0).wait_recv()

        @pl.when(n == 1)
        def _():
            load(x.at[pl.ds(half, half)], 0).start()
            give_own(1).wait_recv()
            load(xg.at[slab(z, 1, 1 - c)], 1).start()

        @pl.when(n > 1)
        def _():
            load(xg.at[slab(j, h, c)], 0).start()
            spot = xg.at[slab(j, h, 1 - c)]
            remote(spot, spot, dd_s.at[came], dd_r.at[jnp.where(came == 0, slot, 2 * CHIPS - 3 - slot)], other).wait_recv()
            load(spot, 1).start()

        load(xg.at[0], 0).wait()

        @pl.when(n > 0)
        def _():
            load(xg.at[0], 1).wait()

        hs = hidden_slot(n)

        @pl.loop(0, TILES)
        def _(i):
            @pl.when(n == 0)
            def _():
                weight(0, wg, wgv, i).wait()
                weight(1, wu, wuv, i).wait()

            gate = jnp.dot(xb[...], wgv[:, cols(i, tile)], preferred_element_type=f32)
            up = jnp.dot(xb[...], wuv[:, cols(i, tile)], preferred_element_type=f32)
            hid[hs, :, cols(i, tile)] = (jax.nn.silu(gate) * up).astype(bf16)

    def relay(s, i):
        for d in range(2):
            @pl.when((s >= 0) & (s < 2 * pos[d]))
            def _():
                p = pos[d] - 1
                j = jnp.where(s <= p, p - s, s - p - 1)
                h = jnp.where(s <= p, 0, 1)
                spot = xg.at[slab(j if d == 0 else CHIPS - 1 - j, h, c), rows(i)]
                remote(spot, spot, ag_s.at[d], ag_r.at[place(d, s), i], ahead[d]).wait_recv()

                @pl.when(pos[d] < CHIPS - 1)
                def _():
                    remote(spot, spot, ag_s.at[d], ag_r.at[place(d, s + 1), i], ahead[d]).start()

                remote(spot, spot, dd_s.at[d], dd_r.at[place(d, s)], other).start()

    def exchange(b, i):
        return remote(give.at[b, i % GIVES], take.at[b, i], give_s.at[b, i % GIVES], take_r.at[b, i], other)

    def make_term(b, hs, i):
        value = jnp.dot(hid[hs], wdv[:, cols(i, width)], preferred_element_type=f32)
        term[b, i % RING] = value[:half]

        @pl.when(i >= GIVES)
        def _():
            exchange(b, i - GIVES).wait_send()

        give[b, i % GIVES] = value[half:].astype(bf16)
        exchange(b, i).start()

    def drain(b):
        for i in range(CHUNKS - GIVES, CHUNKS):
            exchange(b, i).wait_send()

    def to_ring(d, i):
        return remote(snd.at[d, i], rin.at[d, i], snd_s.at[d, i], rin_r.at[d, i], ahead[d])

    def to_own(d, i):
        return remote(snd.at[d, i], own0.at[d, i], snd_s.at[d, i], own_r.at[d], ahead[d])

    def scatter(s):
        active = [(pos[d] < CHIPS - 1) & (s >= 2 * pos[d] + 1) & (s < 7) for d in range(2)]

        @pl.when(active[0] | active[1])
        def _():
            @pl.loop(0, CHUNKS + LAG + HOLD)
            def _(i):
                for d in range(2):
                    far = low if d == 0 else jnp.logical_not(low)

                    @pl.when(active[d] & (i < CHUNKS))
                    def _():
                        make_term(d, hidden_slot(s + 1 - jnp.where(far, 2 * inner, 0)), i)

                for d in range(2):
                    @pl.when(active[d] & (i >= LAG) & (i < CHUNKS + LAG))
                    def _():
                        k = i - LAG
                        exchange(d, k).wait_recv()

                        @pl.when(pos[d] > 0)
                        def _():
                            to_ring(d, k).wait_recv()
                            term[d, k % RING] = term[d, k % RING] + rin[d, k].astype(f32)
                            pl.semaphore_signal(credit.at[d], inc=1, device_id={"tp": behind[d]}, device_id_type=MESH)

                for d in range(2):
                    @pl.when(active[d] & (i >= LAG) & (i < CHUNKS + LAG))
                    def _():
                        k = i - LAG

                        @pl.when(s - 2 * pos[d] - 1 >= 1)
                        def _():
                            to_ring(d, k).wait_send()

                        snd[d, k] = (term[d, k % RING] + take[d, k].astype(f32)).astype(bf16)

                for d in range(2):
                    @pl.when(active[d] & (i >= LAG + HOLD))
                    def _():
                        k = i - LAG - HOLD
                        r = s - 2 * pos[d] - 1

                        @pl.when(r == 0)
                        def _():
                            to_own(d, k).start()

                        @pl.when(r >= 2)
                        def _():
                            pl.semaphore_wait(credit.at[d], 1)

                        @pl.when(r >= 1)
                        def _():
                            to_ring(d, k).start()

            for d in range(2):
                @pl.when(active[d])
                def _():
                    drain(d)

    def finish(h, hs):
        came = own0 if h == 0 else rin
        if h == 0:
            for d in range(2):
                @pl.when(pos[d] > 0)
                def _():
                    remote(own0.at[d], own0.at[d], snd_s.at[d, 0], own_r.at[d], ahead[d]).wait_recv()

        @pl.loop(0, CHUNKS + LAG)
        def _(i):
            @pl.when(i < CHUNKS)
            def _():
                make_term(h, hs, i)

            @pl.when(i >= LAG)
            def _():
                k = i - LAG
                exchange(h, k).wait_recv()
                term[h, k % RING] = term[h, k % RING] + take[h, k].astype(f32)
                for d in range(2):
                    @pl.when(pos[d] > 0)
                    def _():
                        if h == 1:
                            to_ring(d, k).wait_recv()
                        term[h, k % RING] = term[h, k % RING] + came[d, k].astype(f32)

                xb[pl.ds(h * half, half), cols(k, width)] = term[h, k % RING].astype(bf16)

        drain(h)

    @pl.loop(0, 8)
    def _(n):
        s = n - 1
        for d in range(2):
            @pl.when((pos[d] < CHIPS - 1) & (s == 2 * pos[d]))
            def _():
                for i in range(SUBS):
                    send_own(d, 1, s + 1, i).start()

        @pl.when(n == 1)
        def _():
            relay(0, 0)

        forward(n)

        @pl.when(n == 1)
        def _():
            load_wd.wait()

        @pl.when(n > 1)
        def _():
            relay(s, 0)

        scatter(s)
        for i in range(1, SUBS):
            relay(s, i)

    pltpu.make_async_copy(x, x, os).wait()
    for d in range(2):
        for p in range(CHIPS):
            @pl.when(pos[d] == p)
            def _():
                if p < CHIPS - 1:
                    spot = xg.at[pl.ds(0, 2 * p + 2)]
                    remote(spot, spot, ag_s.at[d], ag_r.at[0, 0], ahead[d]).wait_send()
                if p > 0:
                    spot = xg.at[pl.ds(0, 2 * p)]
                    remote(spot, spot, dd_s.at[d], dd_r.at[0], other).wait_send()

    finish(0, 0)
    finish(1, 1)
    for d in range(2):
        @pl.when(pos[d] < CHIPS - 1)
        def _():
            @pl.loop(0, CHUNKS)
            def _(i):
                to_ring(d, i).wait_send()


def block(x, w_gate, w_up, w_down):
    (n, depth), hidden = x.shape, w_gate.shape[1]
    half, width = n // 2, depth // CHUNKS
    f32, bf16, sem = jnp.float32, jnp.bfloat16, pltpu.SemaphoreType
    return pl.pallas_call(
        kernel,
        name="mlp_line",
        out_shape=(
            pltpu.VMEM((n, depth), bf16),
            jax.ShapeDtypeStruct((4 * CHIPS, half, depth), bf16),
        ),
        in_specs=[pl.BlockSpec(memory_space=pl.ANY)] * 4,
        out_specs=(pl.BlockSpec(memory_space=pltpu.VMEM), pl.BlockSpec(memory_space=pl.ANY)),
        scratch_shapes=[
            pltpu.VMEM((depth, hidden), bf16),
            pltpu.VMEM((depth, hidden), bf16),
            pltpu.VMEM((hidden, depth), bf16),
            pltpu.VMEM((5, n, hidden), bf16),
            pltpu.VMEM((2, CHUNKS, half, width), bf16),
            pltpu.VMEM((2, CHUNKS, half, width), bf16),
            pltpu.VMEM((2, CHUNKS, half, width), bf16),
            pltpu.VMEM((2, RING, half, width), f32),
            pltpu.VMEM((2, GIVES, half, width), bf16),
            pltpu.VMEM((2, CHUNKS, half, width), bf16),
            sem.DMA((2,)),
            sem.DMA((6, SUBS)),
            sem.DMA((2,)),
            sem.DMA((6,)),
            sem.DMA,
            sem.DMA((2,)),
            sem.DMA((2, CHUNKS)),
            sem.DMA((2,)),
            sem.DMA((2, CHUNKS)),
            sem.DMA((2, GIVES)),
            sem.DMA((2, CHUNKS)),
            sem.DMA((2 * TILES + 1,)),
            sem.DMA((2,)),
            sem.REGULAR((2,)),
            sem.REGULAR,
        ],
        compiler_params=pltpu.CompilerParams(
            collective_id=0, has_side_effects=True, vmem_limit_bytes=64_700_000
        ),
    )(x, w_gate, w_up, w_down)[0]


def solution(mesh):
    return jax.shard_map(
        block,
        mesh=mesh,
        in_specs=(P(("dp", "tp"), None), P(None, "tp"), P(None, "tp"), P("tp", None)),
        out_specs=P(("dp", "tp"), None),
        check_vma=False,
    )
```

```python
import jax
import jax.numpy as jnp
from jax import lax
from jax.experimental import pallas as pl
from jax.experimental.pallas import tpu as pltpu
from jax.sharding import PartitionSpec as P

MESH = pl.DeviceIdType.MESH
CHIPS = 4
SUBS = 2
CHUNKS = 5
LAG = 1
HOLD = 1
RING = 2
GIVES = 1
TILES = 3


def kernel(
    x, wg, wu, wd, xb, xg,
    wgv, wuv, wdv, hid, rin, own0, snd, term, give, take,
    ag_s, ag_r, dd_s, dd_r, os, orr, rin_r, own_r, snd_s, give_s, take_r, w_s, x_s, credit, hello,
):
    f32, bf16 = jnp.float32, jnp.bfloat16
    half, depth = x.shape[0] // 2, x.shape[1]
    piece, width, tile = half // SUBS, depth // CHUNKS, wg.shape[1] // TILES
    t = lax.axis_index("tp")
    z, c = t // 2, t % 2
    other = t + 1 - 2 * c
    pos = (z, CHIPS - 1 - z)
    ahead, behind = (t + 2, t - 2), (t - 2, t + 2)
    inner = jnp.minimum(z, CHIPS - 1 - z)
    low = z < 2

    def remote(src, dst, send, recv, device):
        return pltpu.make_async_remote_copy(
            src_ref=src, dst_ref=dst, send_sem=send, recv_sem=recv, device_id={"tp": device}, device_id_type=MESH
        )

    def slab(j, h, core):
        return (j * 2 + h) * 2 + core

    def place(d, slot):
        return slot if d == 0 else 2 * CHIPS - 3 - slot

    def rows(i):
        return pl.ds(i * piece, piece)

    def cols(i, n):
        return pl.ds(pl.multiple_of(i * n, n), n)

    def give_own(h):
        spot = xb.at[pl.ds(half, half)] if h == 0 else xg.at[slab(z, h, c)]
        return remote(x.at[pl.ds(h * half, half)], spot, os, orr.at[h], other)

    def load(src, i):
        return pltpu.make_async_copy(src, xb.at[pl.ds(i * half, half)], x_s.at[i])

    def weight(k, src, dst, i):
        return pltpu.make_async_copy(src.at[:, cols(i, tile)], dst.at[:, cols(i, tile)], w_s.at[k * TILES + i])

    barrier = pltpu.get_barrier_semaphore()

    @pl.when(z < CHIPS - 1)
    def _():
        pl.semaphore_signal(barrier, inc=1, device_id={"tp": ahead[0]}, device_id_type=MESH)

    pl.semaphore_signal(barrier, inc=1, device_id={"tp": other}, device_id_type=MESH)
    load(x.at[pl.ds(0, half)], 0).start()
    for i in range(TILES):
        weight(0, wg, wgv, i).start()
        weight(1, wu, wuv, i).start()
    load_wd = pltpu.make_async_copy(wd, wdv, w_s.at[2 * TILES])
    load_wd.start()
    def send_own(d, h, slot, i):
        return remote(
            x.at[pl.ds(h * half + i * piece, piece)], xg.at[slab(z, h, c), rows(i)],
            ag_s.at[d], ag_r.at[place(d, slot), i], ahead[d],
        )

    pl.semaphore_wait(barrier, 1 + jnp.minimum(z, 1))

    @pl.when(z > 0)
    def _():
        pl.semaphore_signal(hello, inc=1, device_id={"tp": ahead[1]}, device_id_type=MESH)

    late = (c == 1) & (z == 1)

    @pl.when((z > 0) & jnp.logical_not(late))
    def _():
        for i in range(SUBS):
            send_own(1, 0, 0, i).start()

    give_own(0).start()
    give_own(1).start()

    @pl.when(z < CHIPS - 1)
    def _():
        pl.semaphore_wait(hello, 1)
        for i in range(SUBS):
            send_own(0, 0, 0, i).start()

    @pl.when(late)
    def _():
        for i in range(SUBS):
            send_own(1, 0, 0, i).start()


    def hidden_slot(a):
        return jnp.where(a < 2, a, 2 + (a - 2) % 3)

    def forward(n):
        s = n - 1
        far = CHIPS - 1 - inner
        j = jnp.where(s <= far, inner + s, inner + 2 * far + 1 - s)
        h = jnp.where(s <= far, 0, 1)
        near = s > 2 * far
        j = jnp.where(near, 0, j)
        h = jnp.where(near, s - 5, h)
        slot = jnp.where(near, s - 5, s - 1)
        j = jnp.where(low, j, CHIPS - 1 - j)
        came = jnp.where(low, 1, 0)
        came = jnp.where(near, 1 - came, came)

        @pl.when(n == 0)
        def _():
            give_own(0).wait_recv()

        @pl.when(n == 1)
        def _():
            load(x.at[pl.ds(half, half)], 0).start()
            give_own(1).wait_recv()
            load(xg.at[slab(z, 1, 1 - c)], 1).start()

        @pl.when(n > 1)
        def _():
            load(xg.at[slab(j, h, c)], 0).start()
            spot = xg.at[slab(j, h, 1 - c)]
            remote(spot, spot, dd_s.at[came], dd_r.at[jnp.where(came == 0, slot, 2 * CHIPS - 3 - slot)], other).wait_recv()
            load(spot, 1).start()

        load(xg.at[0], 0).wait()

        @pl.when(n > 0)
        def _():
            load(xg.at[0], 1).wait()

        hs = hidden_slot(n)

        @pl.loop(0, TILES)
        def _(i):
            @pl.when(n == 0)
            def _():
                weight(0, wg, wgv, i).wait()
                weight(1, wu, wuv, i).wait()

            gate = jnp.dot(xb[...], wgv[:, cols(i, tile)], preferred_element_type=f32)
            up = jnp.dot(xb[...], wuv[:, cols(i, tile)], preferred_element_type=f32)
            hid[hs, :, cols(i, tile)] = (jax.nn.silu(gate) * up).astype(bf16)

    def relay(s, i):
        for d in range(2):
            @pl.when((s >= 0) & (s < 2 * pos[d]))
            def _():
                p = pos[d] - 1
                j = jnp.where(s <= p, p - s, s - p - 1)
                h = jnp.where(s <= p, 0, 1)
                spot = xg.at[slab(j if d == 0 else CHIPS - 1 - j, h, c), rows(i)]
                remote(spot, spot, ag_s.at[d], ag_r.at[place(d, s), i], ahead[d]).wait_recv()

                @pl.when(pos[d] < CHIPS - 1)
                def _():
                    remote(spot, spot, ag_s.at[d], ag_r.at[place(d, s + 1), i], ahead[d]).start()

                remote(spot, spot, dd_s.at[d], dd_r.at[place(d, s)], other).start()

    def exchange(b, i):
        return remote(give.at[b, i % GIVES], take.at[b, i], give_s.at[b, i % GIVES], take_r.at[b, i], other)

    def make_term(b, hs, i):
        @pl.when(i >= GIVES)
        def _():
            exchange(b, i - GIVES).wait_send()

        for part in range(2):
            value = jnp.dot(hid[hs], wdv[:, cols(2 * i + part, width // 2)], preferred_element_type=f32)
            spot = pl.ds(part * width // 2, width // 2)
            term[b, i % RING, :, spot] = value[:half]
            give[b, i % GIVES, :, spot] = value[half:].astype(bf16)
        exchange(b, i).start()

    def drain(b):
        for i in range(CHUNKS - GIVES, CHUNKS):
            exchange(b, i).wait_send()

    def to_ring(d, i):
        return remote(snd.at[d, i], rin.at[d, i], snd_s.at[d, i], rin_r.at[d, i], ahead[d])

    def to_own(d, i):
        return remote(snd.at[d, i], own0.at[d, i], snd_s.at[d, i], own_r.at[d], ahead[d])

    def scatter(s):
        active = [(pos[d] < CHIPS - 1) & (s >= 2 * pos[d] + 1) & (s < 7) for d in range(2)]

        @pl.when(active[0] | active[1])
        def _():
            @pl.loop(0, CHUNKS + LAG + HOLD)
            def _(i):
                for d in range(2):
                    far = low if d == 0 else jnp.logical_not(low)

                    @pl.when(active[d] & (i < CHUNKS))
                    def _():
                        make_term(d, hidden_slot(s + 1 - jnp.where(far, 2 * inner, 0)), i)

                for d in range(2):
                    @pl.when(active[d] & (i >= LAG) & (i < CHUNKS + LAG))
                    def _():
                        k = i - LAG
                        exchange(d, k).wait_recv()

                        @pl.when(pos[d] > 0)
                        def _():
                            to_ring(d, k).wait_recv()
                            term[d, k % RING] = term[d, k % RING] + rin[d, k].astype(f32)
                            pl.semaphore_signal(credit.at[d], inc=1, device_id={"tp": behind[d]}, device_id_type=MESH)

                for d in range(2):
                    @pl.when(active[d] & (i >= LAG) & (i < CHUNKS + LAG))
                    def _():
                        k = i - LAG

                        @pl.when(s - 2 * pos[d] - 1 >= 1)
                        def _():
                            to_ring(d, k).wait_send()

                        snd[d, k] = (term[d, k % RING] + take[d, k].astype(f32)).astype(bf16)

                for d in range(2):
                    @pl.when(active[d] & (i >= LAG + HOLD))
                    def _():
                        k = i - LAG - HOLD
                        r = s - 2 * pos[d] - 1

                        @pl.when(r == 0)
                        def _():
                            to_own(d, k).start()

                        @pl.when(r >= 2)
                        def _():
                            pl.semaphore_wait(credit.at[d], 1)

                        @pl.when(r >= 1)
                        def _():
                            to_ring(d, k).start()

            for d in range(2):
                @pl.when(active[d])
                def _():
                    drain(d)

    def finish(h, hs):
        came = own0 if h == 0 else rin
        if h == 0:
            for d in range(2):
                @pl.when(pos[d] > 0)
                def _():
                    remote(own0.at[d], own0.at[d], snd_s.at[d, 0], own_r.at[d], ahead[d]).wait_recv()

        @pl.loop(0, CHUNKS + LAG)
        def _(i):
            @pl.when(i < CHUNKS)
            def _():
                make_term(h, hs, i)

            @pl.when(i >= LAG)
            def _():
                k = i - LAG
                exchange(h, k).wait_recv()
                term[h, k % RING] = term[h, k % RING] + take[h, k].astype(f32)
                for d in range(2):
                    @pl.when(pos[d] > 0)
                    def _():
                        if h == 1:
                            to_ring(d, k).wait_recv()
                        term[h, k % RING] = term[h, k % RING] + came[d, k].astype(f32)

                xb[pl.ds(h * half, half), cols(k, width)] = term[h, k % RING].astype(bf16)

        drain(h)

    @pl.loop(0, 8)
    def _(n):
        s = n - 1
        for d in range(2):
            @pl.when((pos[d] < CHIPS - 1) & (s == 2 * pos[d]))
            def _():
                for i in range(SUBS):
                    send_own(d, 1, s + 1, i).start()

        @pl.when(n == 1)
        def _():
            relay(0, 0)

        forward(n)

        @pl.when(n == 1)
        def _():
            load_wd.wait()

        @pl.when(n > 1)
        def _():
            relay(s, 0)

        scatter(s)
        for i in range(1, SUBS):
            relay(s, i)

    pltpu.make_async_copy(x, x, os).wait()
    for d in range(2):
        for p in range(CHIPS):
            @pl.when(pos[d] == p)
            def _():
                if p < CHIPS - 1:
                    spot = xg.at[pl.ds(0, 2 * p + 2)]
                    remote(spot, spot, ag_s.at[d], ag_r.at[0, 0], ahead[d]).wait_send()
                if p > 0:
                    spot = xg.at[pl.ds(0, 2 * p)]
                    remote(spot, spot, dd_s.at[d], dd_r.at[0], other).wait_send()

    finish(0, 0)
    finish(1, 1)
    for d in range(2):
        @pl.when(pos[d] < CHIPS - 1)
        def _():
            @pl.loop(0, CHUNKS)
            def _(i):
                to_ring(d, i).wait_send()


def block(x, w_gate, w_up, w_down):
    (n, depth), hidden = x.shape, w_gate.shape[1]
    half, width = n // 2, depth // CHUNKS
    f32, bf16, sem = jnp.float32, jnp.bfloat16, pltpu.SemaphoreType
    return pl.pallas_call(
        kernel,
        name="mlp_line",
        out_shape=(
            pltpu.VMEM((n, depth), bf16),
            jax.ShapeDtypeStruct((4 * CHIPS, half, depth), bf16),
        ),
        in_specs=[pl.BlockSpec(memory_space=pl.ANY)] * 4,
        out_specs=(pl.BlockSpec(memory_space=pltpu.VMEM), pl.BlockSpec(memory_space=pl.ANY)),
        scratch_shapes=[
            pltpu.VMEM((depth, hidden), bf16),
            pltpu.VMEM((depth, hidden), bf16),
            pltpu.VMEM((hidden, depth), bf16),
            pltpu.VMEM((5, n, hidden), bf16),
            pltpu.VMEM((2, CHUNKS, half, width), bf16),
            pltpu.VMEM((2, CHUNKS, half, width), bf16),
            pltpu.VMEM((2, CHUNKS, half, width), bf16),
            pltpu.VMEM((2, RING, half, width), f32),
            pltpu.VMEM((2, GIVES, half, width), bf16),
            pltpu.VMEM((2, CHUNKS, half, width), bf16),
            sem.DMA((2,)),
            sem.DMA((6, SUBS)),
            sem.DMA((2,)),
            sem.DMA((6,)),
            sem.DMA,
            sem.DMA((2,)),
            sem.DMA((2, CHUNKS)),
            sem.DMA((2,)),
            sem.DMA((2, CHUNKS)),
            sem.DMA((2, GIVES)),
            sem.DMA((2, CHUNKS)),
            sem.DMA((2 * TILES + 1,)),
            sem.DMA((2,)),
            sem.REGULAR((2,)),
            sem.REGULAR,
        ],
        compiler_params=pltpu.CompilerParams(
            collective_id=0, has_side_effects=True, vmem_limit_bytes=64_700_000
        ),
    )(x, w_gate, w_up, w_down)[0]


def solution(mesh):
    return jax.shard_map(
        block,
        mesh=mesh,
        in_specs=(P(("dp", "tp"), None), P(None, "tp"), P(None, "tp"), P("tp", None)),
        out_specs=P(("dp", "tp"), None),
        check_vma=False,
    )
```

```python
import jax
import jax.numpy as jnp
from jax import lax
from jax.experimental import pallas as pl
from jax.experimental.pallas import tpu as pltpu
from jax.sharding import PartitionSpec as P

MESH = pl.DeviceIdType.MESH
CHIPS = 4
SUBS = 2
CHUNKS = 5
LAG = 1
HOLD = 1
RING = 2
GIVES = 1
TILES = 3


def kernel(
    x, wg, wu, wd, xb, xg,
    wgv, wuv, wdv, hid, rin, own0, snd, term, give, take,
    ag_s, ag_r, dd_s, dd_r, os, orr, rin_r, own_r, snd_s, give_s, take_r, w_s, x_s, credit, hello, beside,
):
    f32, bf16 = jnp.float32, jnp.bfloat16
    half, depth = x.shape[0] // 2, x.shape[1]
    piece, width, tile = half // SUBS, depth // CHUNKS, wg.shape[1] // TILES
    t = lax.axis_index("tp")
    z, c = t // 2, t % 2
    other = t + 1 - 2 * c
    pos = (z, CHIPS - 1 - z)
    ahead, behind = (t + 2, t - 2), (t - 2, t + 2)
    inner = jnp.minimum(z, CHIPS - 1 - z)
    low = z < 2

    def remote(src, dst, send, recv, device):
        return pltpu.make_async_remote_copy(
            src_ref=src, dst_ref=dst, send_sem=send, recv_sem=recv, device_id={"tp": device}, device_id_type=MESH
        )

    def slab(j, h, core):
        return (j * 2 + h) * 2 + core

    def place(d, slot):
        return slot if d == 0 else 2 * CHIPS - 3 - slot

    def rows(i):
        return pl.ds(i * piece, piece)

    def cols(i, n):
        return pl.ds(pl.multiple_of(i * n, n), n)

    def give_own(h):
        spot = xb.at[pl.ds(half, half)] if h == 0 else xg.at[slab(z, h, c)]
        return remote(x.at[pl.ds(h * half, half)], spot, os, orr.at[h], other)

    def load(src, i):
        return pltpu.make_async_copy(src, xb.at[pl.ds(i * half, half)], x_s.at[i])

    def weight(k, src, dst, i):
        return pltpu.make_async_copy(src.at[:, cols(i, tile)], dst.at[:, cols(i, tile)], w_s.at[k * TILES + i])

    barrier = pltpu.get_barrier_semaphore()

    @pl.when(z < CHIPS - 1)
    def _():
        pl.semaphore_signal(barrier, inc=1, device_id={"tp": ahead[0]}, device_id_type=MESH)

    @pl.when(c == 1)
    def _():
        pl.semaphore_signal(barrier, inc=1, device_id={"tp": other}, device_id_type=MESH)

    load(x.at[pl.ds(0, half)], 0).start()
    for i in range(TILES):
        weight(0, wg, wgv, i).start()
        weight(1, wu, wuv, i).start()
    load_wd = pltpu.make_async_copy(wd, wdv, w_s.at[2 * TILES])
    load_wd.start()
    def send_own(d, h, slot, i):
        return remote(
            x.at[pl.ds(h * half + i * piece, piece)], xg.at[slab(z, h, c), rows(i)],
            ag_s.at[d], ag_r.at[place(d, slot), i], ahead[d],
        )

    @pl.when((c == 0) | (z > 0))
    def _():
        pl.semaphore_wait(barrier, 1 - c + jnp.minimum(z, 1))


    @pl.when(z > 0)
    def _():
        pl.semaphore_signal(hello, inc=1, device_id={"tp": ahead[1]}, device_id_type=MESH)

    late = (c == 1) & (z == 1)

    def first(start, count):
        return remote(
            x.at[pl.ds(start, count)], xg.at[slab(z, 0, c), pl.ds(start, count)],
            ag_s.at[1], ag_r.at[place(1, 0), 0], ahead[1],
        )

    @pl.when((z > 0) & jnp.logical_not(late))
    def _():
        for i in range(SUBS):
            send_own(1, 0, 0, i).start()

    head = piece // 4 // 8 * 8

    @pl.when(late)
    def _():
        first(0, head).start()

    @pl.when(c == 0)
    def _():
        pl.semaphore_signal(beside, inc=1, device_id={"tp": other}, device_id_type=MESH)

    @pl.when(c == 1)
    def _():
        pl.semaphore_wait(beside, 1)

    give_own(0).start()
    give_own(1).start()

    @pl.when(z < CHIPS - 1)
    def _():
        pl.semaphore_wait(hello, 1)
        for i in range(SUBS):
            send_own(0, 0, 0, i).start()


    def hidden_slot(a):
        return jnp.where(a < 2, a, 2 + (a - 2) % 3)

    def forward(n):
        s = n - 1
        far = CHIPS - 1 - inner
        j = jnp.where(s <= far, inner + s, inner + 2 * far + 1 - s)
        h = jnp.where(s <= far, 0, 1)
        near = s > 2 * far
        j = jnp.where(near, 0, j)
        h = jnp.where(near, s - 5, h)
        slot = jnp.where(near, s - 5, s - 1)
        j = jnp.where(low, j, CHIPS - 1 - j)
        came = jnp.where(low, 1, 0)
        came = jnp.where(near, 1 - came, came)

        @pl.when(n == 0)
        def _():
            give_own(0).wait_recv()

        @pl.when(n == 1)
        def _():
            load(x.at[pl.ds(half, half)], 0).start()
            give_own(1).wait_recv()
            load(xg.at[slab(z, 1, 1 - c)], 1).start()

        @pl.when(n > 1)
        def _():
            load(xg.at[slab(j, h, c)], 0).start()
            spot = xg.at[slab(j, h, 1 - c)]
            remote(spot, spot, dd_s.at[came], dd_r.at[jnp.where(came == 0, slot, 2 * CHIPS - 3 - slot)], other).wait_recv()
            load(spot, 1).start()

        load(xg.at[0], 0).wait()

        @pl.when(n > 0)
        def _():
            load(xg.at[0], 1).wait()

        hs = hidden_slot(n)

        @pl.loop(0, TILES)
        def _(i):
            @pl.when(n == 0)
            def _():
                weight(0, wg, wgv, i).wait()
                weight(1, wu, wuv, i).wait()

                @pl.when(late & (i == 0))
                def _():
                    first(head, piece - head).start()
                    for k in range(1, SUBS):
                        send_own(1, 0, 0, k).start()

            gate = jnp.dot(xb[...], wgv[:, cols(i, tile)], preferred_element_type=f32)
            up = jnp.dot(xb[...], wuv[:, cols(i, tile)], preferred_element_type=f32)
            hid[hs, :, cols(i, tile)] = (jax.nn.silu(gate) * up).astype(bf16)

    def relay(s, i):
        for d in range(2):
            @pl.when((s >= 0) & (s < 2 * pos[d]))
            def _():
                p = pos[d] - 1
                j = jnp.where(s <= p, p - s, s - p - 1)
                h = jnp.where(s <= p, 0, 1)
                spot = xg.at[slab(j if d == 0 else CHIPS - 1 - j, h, c), rows(i)]
                remote(spot, spot, ag_s.at[d], ag_r.at[place(d, s), i], ahead[d]).wait_recv()

                @pl.when(pos[d] < CHIPS - 1)
                def _():
                    remote(spot, spot, ag_s.at[d], ag_r.at[place(d, s + 1), i], ahead[d]).start()

                remote(spot, spot, dd_s.at[d], dd_r.at[place(d, s)], other).start()

    def exchange(b, i):
        return remote(give.at[b, i % GIVES], take.at[b, i], give_s.at[b, i % GIVES], take_r.at[b, i], other)

    def make_term(b, hs, i):
        @pl.when(i >= GIVES)
        def _():
            exchange(b, i - GIVES).wait_send()

        for part in range(2):
            value = jnp.dot(hid[hs], wdv[:, cols(2 * i + part, width // 2)], preferred_element_type=f32)
            spot = pl.ds(part * width // 2, width // 2)
            term[b, i % RING, :, spot] = value[:half]
            give[b, i % GIVES, :, spot] = value[half:].astype(bf16)
        exchange(b, i).start()

    def drain(b):
        for i in range(CHUNKS - GIVES, CHUNKS):
            exchange(b, i).wait_send()

    def to_ring(d, i):
        return remote(snd.at[d, i], rin.at[d, i], snd_s.at[d, i], rin_r.at[d, i], ahead[d])

    def to_own(d, i):
        return remote(snd.at[d, i], own0.at[d, i], snd_s.at[d, i], own_r.at[d], ahead[d])

    def scatter(s):
        active = [(pos[d] < CHIPS - 1) & (s >= 2 * pos[d] + 1) & (s < 7) for d in range(2)]

        @pl.when(active[0] | active[1])
        def _():
            @pl.loop(0, CHUNKS + LAG + HOLD)
            def _(i):
                for d in range(2):
                    far = low if d == 0 else jnp.logical_not(low)

                    @pl.when(active[d] & (i < CHUNKS))
                    def _():
                        make_term(d, hidden_slot(s + 1 - jnp.where(far, 2 * inner, 0)), i)

                for d in range(2):
                    @pl.when(active[d] & (i >= LAG) & (i < CHUNKS + LAG))
                    def _():
                        k = i - LAG
                        exchange(d, k).wait_recv()

                        @pl.when(pos[d] > 0)
                        def _():
                            to_ring(d, k).wait_recv()
                            term[d, k % RING] = term[d, k % RING] + rin[d, k].astype(f32)
                            pl.semaphore_signal(credit.at[d], inc=1, device_id={"tp": behind[d]}, device_id_type=MESH)

                for d in range(2):
                    @pl.when(active[d] & (i >= LAG) & (i < CHUNKS + LAG))
                    def _():
                        k = i - LAG

                        @pl.when(s - 2 * pos[d] - 1 >= 1)
                        def _():
                            to_ring(d, k).wait_send()

                        snd[d, k] = (term[d, k % RING] + take[d, k].astype(f32)).astype(bf16)

                for d in range(2):
                    @pl.when(active[d] & (i >= LAG + HOLD))
                    def _():
                        k = i - LAG - HOLD
                        r = s - 2 * pos[d] - 1

                        @pl.when(r == 0)
                        def _():
                            to_own(d, k).start()

                        @pl.when(r >= 2)
                        def _():
                            pl.semaphore_wait(credit.at[d], 1)

                        @pl.when(r >= 1)
                        def _():
                            to_ring(d, k).start()

            for d in range(2):
                @pl.when(active[d])
                def _():
                    drain(d)

    def finish(h, hs):
        came = own0 if h == 0 else rin
        if h == 0:
            for d in range(2):
                @pl.when(pos[d] > 0)
                def _():
                    remote(own0.at[d], own0.at[d], snd_s.at[d, 0], own_r.at[d], ahead[d]).wait_recv()

        @pl.loop(0, CHUNKS + LAG)
        def _(i):
            @pl.when(i < CHUNKS)
            def _():
                make_term(h, hs, i)

            @pl.when(i >= LAG)
            def _():
                k = i - LAG
                exchange(h, k).wait_recv()
                term[h, k % RING] = term[h, k % RING] + take[h, k].astype(f32)
                for d in range(2):
                    @pl.when(pos[d] > 0)
                    def _():
                        if h == 1:
                            to_ring(d, k).wait_recv()
                        term[h, k % RING] = term[h, k % RING] + came[d, k].astype(f32)

                xb[pl.ds(h * half, half), cols(k, width)] = term[h, k % RING].astype(bf16)

        drain(h)

    @pl.loop(0, 8)
    def _(n):
        s = n - 1
        for d in range(2):
            @pl.when((pos[d] < CHIPS - 1) & (s == 2 * pos[d]))
            def _():
                for i in range(SUBS):
                    send_own(d, 1, s + 1, i).start()

        @pl.when(n == 1)
        def _():
            relay(0, 0)

        forward(n)

        @pl.when(n == 1)
        def _():
            load_wd.wait()

        @pl.when(n > 1)
        def _():
            relay(s, 0)

        scatter(s)
        for i in range(1, SUBS):
            relay(s, i)

    pltpu.make_async_copy(x, x, os).wait()
    for d in range(2):
        for p in range(CHIPS):
            @pl.when(pos[d] == p)
            def _():
                if p < CHIPS - 1:
                    spot = xg.at[pl.ds(0, 2 * p + 2)]
                    remote(spot, spot, ag_s.at[d], ag_r.at[0, 0], ahead[d]).wait_send()
                if p > 0:
                    spot = xg.at[pl.ds(0, 2 * p)]
                    remote(spot, spot, dd_s.at[d], dd_r.at[0], other).wait_send()

    finish(0, 0)
    finish(1, 1)
    for d in range(2):
        @pl.when(pos[d] < CHIPS - 1)
        def _():
            @pl.loop(0, CHUNKS)
            def _(i):
                to_ring(d, i).wait_send()


def block(x, w_gate, w_up, w_down):
    (n, depth), hidden = x.shape, w_gate.shape[1]
    half, width = n // 2, depth // CHUNKS
    f32, bf16, sem = jnp.float32, jnp.bfloat16, pltpu.SemaphoreType
    return pl.pallas_call(
        kernel,
        name="mlp_line",
        out_shape=(
            pltpu.VMEM((n, depth), bf16),
            jax.ShapeDtypeStruct((4 * CHIPS, half, depth), bf16),
        ),
        in_specs=[pl.BlockSpec(memory_space=pl.ANY)] * 4,
        out_specs=(pl.BlockSpec(memory_space=pltpu.VMEM), pl.BlockSpec(memory_space=pl.ANY)),
        scratch_shapes=[
            pltpu.VMEM((depth, hidden), bf16),
            pltpu.VMEM((depth, hidden), bf16),
            pltpu.VMEM((hidden, depth), bf16),
            pltpu.VMEM((5, n, hidden), bf16),
            pltpu.VMEM((2, CHUNKS, half, width), bf16),
            pltpu.VMEM((2, CHUNKS, half, width), bf16),
            pltpu.VMEM((2, CHUNKS, half, width), bf16),
            pltpu.VMEM((2, RING, half, width), f32),
            pltpu.VMEM((2, GIVES, half, width), bf16),
            pltpu.VMEM((2, CHUNKS, half, width), bf16),
            sem.DMA((2,)),
            sem.DMA((6, SUBS)),
            sem.DMA((2,)),
            sem.DMA((6,)),
            sem.DMA,
            sem.DMA((2,)),
            sem.DMA((2, CHUNKS)),
            sem.DMA((2,)),
            sem.DMA((2, CHUNKS)),
            sem.DMA((2, GIVES)),
            sem.DMA((2, CHUNKS)),
            sem.DMA((2 * TILES + 1,)),
            sem.DMA((2,)),
            sem.REGULAR((2,)),
            sem.REGULAR,
            sem.REGULAR,
        ],
        compiler_params=pltpu.CompilerParams(
            collective_id=0, has_side_effects=True, vmem_limit_bytes=64_700_000
        ),
    )(x, w_gate, w_up, w_down)[0]


def solution(mesh):
    return jax.shard_map(
        block,
        mesh=mesh,
        in_specs=(P(("dp", "tp"), None), P(None, "tp"), P(None, "tp"), P("tp", None)),
        out_specs=P(("dp", "tp"), None),
        check_vma=False,
    )
```
